32 devices in a mesh: seq: 4 (over y, x), mem: 8 (over z, core).
Axes of the slice: x: 2, y: 2, z: 4, core: 2. Of those that a mesh axis runs over, the one named last changes fastest.
Arguments:
- hidden: bfloat16 [8192, 2048], P(('seq', 'mem')), may hold values from -6 to 6
- routes: int32 [8192, 2], P(('seq', 'mem')), may hold values from 0 to 7, all different within a row; in each aligned block of 256 rows (0 to 255, 256 to 511, ...) at most 64 rows name the same one
- gate_levels: int32 [8192, 2], P(('seq', 'mem')), may hold values from 1 to 255
- query_weight: bfloat16 [2048, 1024], P('seq'), may hold values from -0.125 to 0.125
- key_weight: bfloat16 [8, 2048, 1024], P('mem', 'seq'), may hold values from -0.125 to 0.125
- value_weight: bfloat16 [8, 2048, 1024], P('mem', 'seq'), may hold values from -0.125 to 0.125
Outputs:
- mixed: bfloat16 [8192, 1024], P(('seq', 'mem'))
The draws below stay inside these ranges and needn't reach their ends.
Inputs may be any that keep to these rules, and one draw needn't show every extreme that they name: `routes`: the two memories of a row differ. In the rows of one device no memory is named by more than 64 rows, a bound that some block reaches.
All inputs are finite; a program needn't handle non-finite values.
Results may differ from the reference program's by a relative error of at most 0.01.
Values may be sent and summed in bfloat16 or wider, within the bound.
No kernel may reach another device: no remote copies, remote signals or barrier semaphores. Data moves between devices by JAX's collectives and lax.ppermute only.
A program may use at most 128 MiB of HBM per device.

```python
import math
import jax
import jax.numpy as jnp
import numpy as np
from jax import lax

D = 2048
HEADS = 8
DK = 128
TOK_DEV = 256
BLOCK = 512
CAP = 64
HD = 1024
EXPERTS = 8
TOKENS = 8192


def plant(array, own_key, low, largest):
    dims = array.shape
    place = [jax.random.randint(jax.random.fold_in(own_key, axis), (), 0, dims[axis]) for axis in range(len(dims))]
    array = array.at[tuple(place)].set(low)
    longest = dims.index(max(dims))
    place[longest] = (place[longest] + 1) % dims[longest]
    return array.at[tuple(place)].set(largest)


def shard_levels(rng, dims, cuts, low, top_value):
    gain = 1.0
    for dim, parts in cuts:
        draws = jax.random.uniform(jax.random.fold_in(jax.random.fold_in(rng, 6), dim), (parts,), jnp.float32, low / len(cuts), top_value / len(cuts))
        gain = gain * jnp.repeat(jnp.exp(draws), dims[dim] // parts).reshape((-1,) + (1,) * (len(dims) - 1 - dim))
    return gain


def deal_out(key, own, number, rows, number_of, top, limit, lean):
    order = jax.random.permutation(key, number_of)
    crowded, usual = shares(number_of, rows * top, limit, lean, True), shares(number_of, rows * top, limit, lean, False)
    places = jnp.arange(number_of)

    def named(sizes, turn):
        used = int((sizes > 0).sum())
        fixed = max(1, used // 4)
        passed = fixed + (places - fixed + turn * (used - fixed)) % max(1, number_of - fixed)
        return jnp.zeros((number_of,), jnp.int32).at[order[jnp.where(places < fixed, places, passed)]].set(jnp.asarray(sizes, jnp.int32))

    sizes = jnp.where(number % 4 == 0, named(crowded, number // 4), named(usual, number - number // 4 - 1))
    mixed = jax.random.permutation(jax.random.fold_in(own, 3), number_of)
    donor, taker = mixed[0:number_of // 2 * 2:2], mixed[1:number_of // 2 * 2:2]
    margin = jnp.minimum(sizes[donor] - 1, limit - sizes[taker]) // 2
    margin = jnp.where((donor == order[0]) | (taker == order[0]) | (sizes[taker] == 0), 0, jnp.maximum(margin, 0))
    passed = jax.random.randint(jax.random.fold_in(own, 4), (number_of // 2,), 0, 1 << 20) % (margin + 1)
    sizes = sizes.at[donor].add(-passed).at[taker].add(passed)
    members = jnp.searchsorted(jnp.cumsum(sizes), jnp.arange(rows * top), side="right").astype(jnp.int32)
    grid = members.reshape(top, rows).T
    grid = grid[jax.random.permutation(jax.random.fold_in(own, 1), rows)]
    turn = jax.random.randint(jax.random.fold_in(own, 2), (rows, 1), 0, top)
    return jnp.take_along_axis(grid, (jnp.arange(top)[None, :] + turn) % top, axis=1)


def shares(amount, total, reach, lean, full):
    loads = [(1 << 20) // math.isqrt(rank ** lean) + 1 for rank in range(1, amount + 1)]
    largest = reach if full else min(reach, max(-(-total // amount), total * loads[0] // sum(loads)))
    least = 1 if total - largest >= amount - 1 else 0
    given, surplus = [largest] + [least] * (amount - 1), total - largest - least * (amount - 1)
    while surplus > 0:
        candidates = [i for i in range(1, amount) if given[i] < largest] or [i for i in range(1, amount) if given[i] < reach]
        whole, budget = sum([loads[i] for i in candidates]), surplus
        for i in candidates:
            extra = min(reach - given[i], max(1, budget * loads[i] // whole), surplus)
            given[i] = given[i] + extra
            surplus = surplus - extra
    return np.array(given)


def bell_draw(key, shape, scale, bound, shards=(), kind=jnp.bfloat16):
    loudness = shard_levels(key, shape, shards, -0.22, 0.18) if shards else 1.0
    result = jax.random.normal(key, shape, jnp.float32) * scale * loudness
    return jnp.minimum(jnp.maximum(result, -bound), bound).astype(kind)


def setup_inputs(seed: int = 0) -> dict:
    key_list = jax.random.split(jax.random.key(seed), 7)
    hidden = bell_draw(key_list[0], (TOKENS, D), 1.0, 6.0, ((0, 32),))
    routes_keys = jax.random.split(jax.random.fold_in(key_list[1], 1), TOKENS // TOK_DEV)
    routes_turns = jax.random.permutation(jax.random.fold_in(key_list[1], 3), TOKENS // TOK_DEV)
    routes = jax.vmap(lambda own, number: deal_out(jax.random.fold_in(key_list[1], 2), own, number, TOK_DEV, EXPERTS, 2, CAP, 2))(routes_keys, routes_turns).reshape((TOKENS, 2))
    gate_levels = plant(jax.random.randint(key_list[2], (TOKENS, 2), 1, 256), jax.random.fold_in(key_list[2], 1), 1, 255).astype(jnp.int32)
    query_weight = bell_draw(key_list[3], (D, HD), D ** -0.5, 0.125, ((0, 4),))
    key_weight = bell_draw(key_list[4], (EXPERTS, D, HD), D ** -0.5, 0.125, ((0, 8), (1, 4)))
    value_weight = bell_draw(key_list[5], (EXPERTS, D, HD), D ** -0.5, 0.125, ((0, 8), (1, 4)))
    return dict(hidden=hidden, routes=routes, gate_levels=gate_levels, query_weight=query_weight, key_weight=key_weight, value_weight=value_weight)


def reference(hidden, routes, gate_levels, query_weight, key_weight, value_weight):
    tokens = hidden.shape[0]
    width = query_weight.shape[1]
    highest = lax.Precision.HIGHEST
    queries = jnp.dot(hidden, query_weight, preferred_element_type=jnp.float32).astype(jnp.bfloat16)
    levels = gate_levels.astype(jnp.float32)
    gates = levels / lax.optimization_barrier(jnp.sum(levels, axis=1, keepdims=True))
    padded = tokens // TOK_DEV * CAP
    blocks = padded // BLOCK
    order = jnp.arange(tokens, dtype=jnp.int32)
    rowids = jnp.arange(BLOCK, dtype=jnp.int32)
    causal = (rowids[:, None] >= rowids[None, :]).astype(jnp.float32)

    def step(state, inputs):
        q_block, k_block, v_block = inputs
        scores = jnp.einsum('qhd,khd->hqk', q_block, k_block, precision=highest) * causal[None]
        local = jnp.einsum('hqk,khd->qhd', scores, v_block, precision=highest)
        carried = jnp.einsum('qhd,hde->qhe', q_block, state, precision=highest)
        state = state + jnp.einsum('khd,khe->hde', k_block, v_block, precision=highest)
        return (state, local + carried)

    def memory(expert, total):
        hit = routes == expert
        flag = jnp.any(hit, axis=1)
        keyed = jnp.where(flag, order, order + tokens)
        picked = jnp.argsort(keyed)[:padded].astype(jnp.int32)
        valid = jnp.arange(padded, dtype=jnp.int32) < jnp.sum(flag.astype(jnp.int32))
        chosen = jnp.where(valid[:, None], jnp.take(hidden, picked, axis=0), jnp.zeros((), hidden.dtype))
        w_key = lax.dynamic_index_in_dim(key_weight, expert, 0, keepdims=False)
        w_value = lax.dynamic_index_in_dim(value_weight, expert, 0, keepdims=False)
        keys = jnp.dot(chosen, w_key, preferred_element_type=jnp.float32).astype(jnp.bfloat16)
        values = jnp.dot(chosen, w_value, preferred_element_type=jnp.float32).astype(jnp.bfloat16)
        q_sel = jnp.where(valid[:, None], jnp.take(queries, picked, axis=0), jnp.zeros((), queries.dtype))
        shape4 = (blocks, BLOCK, HEADS, DK)
        q_four = q_sel.astype(jnp.float32).reshape(shape4)
        k_four = keys.astype(jnp.float32).reshape(shape4)
        v_four = values.astype(jnp.float32).reshape(shape4)
        start = jnp.zeros((HEADS, DK, DK), jnp.float32)
        _, reads = lax.scan(step, start, (q_four, k_four, v_four))
        scale = lax.rsqrt(lax.optimization_barrier(jnp.mean(reads * reads, axis=-1, keepdims=True)) + 1e-06)
        normed = (reads * scale).astype(jnp.bfloat16).astype(jnp.float32).reshape(padded, width)
        weight = lax.optimization_barrier(jnp.sum(jnp.where(hit, gates, jnp.zeros((), jnp.float32)), axis=1))
        weight = jnp.where(valid, jnp.take(weight, picked, axis=0), jnp.zeros((), jnp.float32))
        return total.at[picked].add(weight[:, None] * normed)
    total = lax.fori_loop(0, EXPERTS, memory, jnp.zeros((tokens, width), jnp.float32))
    return total.astype(jnp.bfloat16)
```

```python
import functools

import jax
import jax.numpy as jnp
from jax import lax
from jax.experimental import pallas as pl
from jax.experimental.pallas import tpu as pltpu
from jax.sharding import PartitionSpec as P


DK = 128
CAP = 64
LAST_HEADS = 2
LIMIT = 24 << 20
VMEM = pl.BlockSpec(memory_space=pltpu.VMEM)
SMEM = pl.BlockSpec(memory_space=pltpu.SMEM)
ANY = pl.BlockSpec(memory_space=pl.ANY)
HBM = pl.BlockSpec(memory_space=pltpu.HBM)
shape = jax.ShapeDtypeStruct
bf16 = jnp.bfloat16


def swap(array, axis, mask, forward_only=False):
    size = lax.axis_size(axis)
    pairs = [(i, i ^ mask) for i in range(size) if i < i ^ mask or not forward_only]
    return lax.ppermute(array, axis, pairs)


def contract(left, right, left_dim, right_dim):
    return lax.dot_general(
        left, right, (((left_dim,), (right_dim,)), ((), ())), preferred_element_type=jnp.float32
    )


def dispatch_kernel(here, routes, levels, hidden, table, *sent):
    count = hidden.shape[0]
    experts = len(sent)
    named = [routes[j : j + 1, :] for j in range(2)]
    memory = lax.broadcasted_iota(jnp.int32, (experts, count), 0)
    hits = [(memory == name).astype(jnp.float32) for name in named]
    rows = lax.broadcasted_iota(jnp.int32, (count, count), 0)
    cols = lax.broadcasted_iota(jnp.int32, (count, count), 1)
    earlier = jnp.where(rows < cols, 1.0, 0.0).astype(bf16)
    before = contract((hits[0] + hits[1]).astype(bf16), earlier, 1, 0)
    places = [jnp.sum(h * before, axis=0, keepdims=True).astype(jnp.int32) for h in hits]
    index = lax.broadcasted_iota(jnp.int32, (CAP, count), 0)
    crossed = [(name ^ here[1]) * CAP + place for name, place in zip(named, places)]
    for k in range(experts):
        at = index + k * CAP
        pick = jnp.where((at == crossed[0]) | (at == crossed[1]), 1.0, 0.0).astype(bf16)
        sent[k][...] = contract(pick, hidden[...], 1, 0).astype(bf16)
    slots = [(name * CAP + place).astype(jnp.float32) for name, place in zip(named, places)]
    level = levels[...].astype(jnp.float32)
    gates = level / (level[0:1, :] + level[1:2, :])
    entries = jnp.concatenate(slots + [gates, jnp.zeros((4, count), jnp.float32)], axis=0)
    table[...] = entries.T


def pack_kernel(here, query, key, value, a_out, b_out, sems, *, first, heads, a_heads):
    mine = heads // 2
    width = heads * DK
    start = first * DK
    side = here[1] & 1
    q_at = pl.multiple_of((first + side * mine) * DK, DK)
    copies = [
        pltpu.make_async_copy(key.at[0, :, pl.ds(start, width)], a_out.at[:, pl.ds(0, width)], sems.at[0]),
        pltpu.make_async_copy(value.at[0, :, pl.ds(start, width)], b_out.at[:, pl.ds(0, width)], sems.at[1]),
    ]
    a_cols = a_heads * DK
    b_cols = (mine - a_heads) * DK
    if a_cols:
        copies.append(
            pltpu.make_async_copy(
                query.at[:, pl.ds(q_at, a_cols)], a_out.at[:, pl.ds(width, a_cols)], sems.at[2]
            )
        )
    if b_cols:
        copies.append(
            pltpu.make_async_copy(
                query.at[:, pl.ds(pl.multiple_of(q_at + a_cols, DK), b_cols)],
                b_out.at[:, pl.ds(width, b_cols)],
                sems.at[3],
            )
        )
    for copy in copies:
        copy.start()
    for copy in copies:
        copy.wait()


def join_kernel(here, *refs):
    *pieces, out = refs
    for k, piece in enumerate(pieces):
        out[pl.ds(pl.multiple_of((here[1] ^ k) * CAP, CAP), CAP), :] = piece[...]


def project(x, seq, pieces, masks):
    total = None
    for piece, mask in zip(pieces, masks):
        rows = piece.shape[0]
        at = pl.multiple_of((seq ^ mask) * rows, rows)
        part = contract(x[:, pl.ds(at, rows)], piece[...], 1, 0)
        total = part if total is None else total + part
    return total


def kv_kernel(here, x, *refs, masks, heads, a_heads):
    n = len(masks[0])
    k_out, v_out, q_out, t_out, q_pack = refs[2 * n :]
    width = heads * DK
    seq = here[0]
    q_at = 0
    for pieces, own, out, extra in (
        (refs[:n], masks[0], k_out, a_heads * DK),
        (refs[n : 2 * n], masks[1], v_out, (heads // 2 - a_heads) * DK),
    ):
        part = project(x, seq, pieces, own).astype(bf16)
        out[...] = part[:, :width]
        if extra:
            q_out[:, q_at : q_at + extra] = part[:, width:]
            for piece, mask in zip(pieces, own):
                rows = piece.shape[0]
                at = pl.multiple_of((seq ^ mask) * rows, rows)
                q_pack[pl.ds(at, rows), q_at : q_at + extra] = piece[:, width:]
        q_at += extra
    for h in range(heads):
        cols = slice(h * DK, (h + 1) * DK)
        t_out[h] = contract(k_out[:, cols], v_out[:, cols], 0, 0).astype(bf16)


def attend_kernel(here, x, k, v, q_own, w_other, *refs):
    *states, out = refs
    length = x.shape[0]
    side = here[1] & 1
    mine = q_own.shape[1] // DK
    step = length // 2
    row = lax.broadcasted_iota(jnp.int32, (step, step), 0)
    col = lax.broadcasted_iota(jnp.int32, (step, step), 1)
    causal = row >= col
    q_other = contract(x[...], w_other[...], 1, 0).astype(bf16)
    for queries, group in ((q_own, side), (q_other, 1 - side)):
        for h in range(mine):
            head = group * mine + h
            cols = pl.ds(pl.multiple_of(head * DK, DK), DK)
            state = states[0][head].astype(jnp.float32)
            for other in states[1:]:
                state = state + other[head].astype(jnp.float32)
            high = state.astype(bf16)
            low = (state - high.astype(jnp.float32)).astype(bf16)
            for b in range(2):
                rows = slice(b * step, (b + 1) * step)
                q = queries[rows, h * DK : (h + 1) * DK]
                scores = jnp.where(causal, contract(q, k[rows, cols], 1, 1), 0.0).astype(bf16)
                reads = contract(scores, v[rows, cols], 1, 0)
                for e in range(b):
                    earlier = slice(e * step, (e + 1) * step)
                    scores = contract(q, k[earlier, cols], 1, 1).astype(bf16)
                    reads = reads + contract(scores, v[earlier, cols], 1, 0)
                reads = reads + contract(q, high, 1, 0) + contract(q, low, 1, 0)
                scale = lax.rsqrt(jnp.mean(reads * reads, axis=-1, keepdims=True) + 1e-06)
                out[rows, cols] = (reads * scale).astype(bf16)


def combine_kernel(table, part, *refs):
    out = refs[-1]
    count = table.shape[0]
    index = lax.broadcasted_iota(jnp.int32, (count, part.shape[0]), 1).astype(jnp.float32)
    mixed = None
    for j in range(2):
        pick = jnp.where(index == table[:, j : j + 1], 1.0, 0.0).astype(bf16)
        term = table[:, 2 + j : 3 + j] * contract(pick, part[...], 1, 0)
        mixed = term if mixed is None else mixed + term
    out[...] = mixed.astype(bf16)


def call(kernel, outs, ins, *arrays, flops=1, scratch=()):
    arrays = [
        pltpu.with_memory_space_constraint(a, pltpu.VMEM) if spec is VMEM else a
        for a, spec in zip(arrays, ins)
    ]
    return pl.pallas_call(
        kernel,
        out_shape=jax.tree.map(lambda s: pltpu.VMEM(s.shape, s.dtype), outs),
        in_specs=ins,
        out_specs=jax.tree.map(lambda _: VMEM, outs),
        scratch_shapes=scratch,
        compiler_params=pltpu.CompilerParams(vmem_limit_bytes=LIMIT),
        cost_estimate=pl.CostEstimate(flops=flops, bytes_accessed=1 << 20, transcendentals=0),
    )(*arrays)


def spread(first, bits):
    pieces, masks = [first], [0]
    for bit in bits:
        fresh = []
        for piece in pieces:
            fresh.append(swap(piece, "seq", bit))
        pieces = pieces + fresh
        masks = masks + [m ^ bit for m in masks]
    return pieces, tuple(masks)


def on_device(hidden, routes, gate_levels, query_weight, key_weight, value_weight):
    count, model = hidden.shape
    rows, width = query_weight.shape
    groups, experts = lax.axis_size("seq"), lax.axis_size("mem")
    here = jnp.stack([lax.axis_index("seq"), lax.axis_index("mem")]).astype(jnp.int32)
    bits = [1 << b for b in range(groups.bit_length() - 1)]
    length = experts * CAP
    all_heads = width // DK
    chunks = [(0, all_heads - LAST_HEADS), (all_heads - LAST_HEADS, LAST_HEADS)]

    weights = []
    for c, (first, heads) in enumerate(chunks):
        mine = heads // 2
        a_heads = (mine + 1 - c % 2) // 2
        a_cols, b_cols = (heads + a_heads) * DK, (heads + mine - a_heads) * DK
        a_first, b_first = call(
            functools.partial(pack_kernel, first=first, heads=heads, a_heads=a_heads),
            [shape((rows, a_cols), bf16), shape((rows, b_cols), bf16)],
            [SMEM, HBM, HBM, HBM],
            here,
            query_weight,
            key_weight,
            value_weight,
            scratch=[pltpu.SemaphoreType.DMA((4,))],
        )
        a_pieces, a_masks = spread(a_first, bits)
        b_pieces, b_masks = spread(b_first, bits[::-1])
        weights.append((a_pieces, b_pieces, (a_masks, b_masks), a_heads))

    table, *sent = call(
        dispatch_kernel,
        [shape((count, 8), jnp.float32)] + [shape((CAP, model), bf16)] * experts,
        [SMEM, VMEM, VMEM, VMEM],
        here,
        routes.T,
        gate_levels.T,
        hidden,
        flops=2 * count * length * model,
    )

    def route(array, k):
        return swap(array, "mem", k)

    arrived = call(
        join_kernel,
        shape((length, model), bf16),
        [SMEM] + [VMEM] * experts,
        here,
        sent[0],
        *[route(sent[k], k) for k in range(1, experts)],
    )

    out = None
    for c, (first, heads) in enumerate(chunks):
        a_pieces, b_pieces, masks, a_heads = weights[c]
        mine = heads // 2
        cols = heads * DK
        keys, values, q_own, total, q_pack = call(
            functools.partial(kv_kernel, masks=masks, heads=heads, a_heads=a_heads),
            [
                shape((length, cols), bf16),
                shape((length, cols), bf16),
                shape((length, mine * DK), bf16),
                shape((heads, DK, DK), bf16),
                shape((model, mine * DK), bf16),
            ],
            [SMEM, VMEM] + [VMEM] * (2 * groups),
            here,
            arrived,
            *a_pieces,
            *b_pieces,
            flops=4 * length * model * cols,
        )
        states = []
        for m in range(1, groups):
            states.append(swap(total, "seq", m, forward_only=True))
        w_other = swap(q_pack, "mem", 1)
        normed = call(
            attend_kernel,
            shape((length, cols), bf16),
            [SMEM] + [VMEM] * (5 + len(states)),
            here,
            arrived,
            keys,
            values,
            q_own,
            w_other,
            *states,
            flops=4 * length * model * cols,
        )
        back = lax.all_to_all(
            normed.reshape(experts, CAP, cols), "mem", split_axis=0, concat_axis=0, tiled=True
        )
        back = back.reshape(length, cols)
        prior = [] if out is None else [out]
        out = pl.pallas_call(
            combine_kernel,
            grid=(1,),
            out_shape=shape((count, width), bf16),
            in_specs=[
                pl.BlockSpec((count, 8), lambda i: (0, 0)),
                pl.BlockSpec((length, cols), lambda i: (0, 0)),
            ]
            + [ANY] * len(prior),
            out_specs=pl.BlockSpec((count, cols), lambda i, at=first // heads: (0, at)),
            input_output_aliases={2: 0} if prior else {},
        )(table, back, *prior)
    return out


def solution(mesh):
    return jax.shard_map(
        on_device,
        mesh=mesh,
        in_specs=(
            P(("seq", "mem"), None),
            P(("seq", "mem"), None),
            P(("seq", "mem"), None),
            P("seq", None),
            P("mem", "seq", None),
            P("mem", "seq", None),
        ),
        out_specs=P(("seq", "mem"), None),
        check_vma=False,
    )
```

```python
import functools

import jax
import jax.numpy as jnp
from jax import lax
from jax.experimental import pallas as pl
from jax.experimental.pallas import tpu as pltpu
from jax.sharding import PartitionSpec as P


DK = 128
CAP = 64
LAST_HEADS = 3
LIMIT = 24 << 20
VMEM = pl.BlockSpec(memory_space=pltpu.VMEM)
SMEM = pl.BlockSpec(memory_space=pltpu.SMEM)
ANY = pl.BlockSpec(memory_space=pl.ANY)
HBM = pl.BlockSpec(memory_space=pltpu.HBM)
shape = jax.ShapeDtypeStruct
bf16 = jnp.bfloat16


def swap(array, axis, mask):
    return lax.ppermute(array, axis, [(i, i ^ mask) for i in range(lax.axis_size(axis))])


def contract(left, right, left_dim, right_dim):
    return lax.dot_general(
        left, right, (((left_dim,), (right_dim,)), ((), ())), preferred_element_type=jnp.float32
    )


def dispatch_kernel(here, routes, levels, hidden, table, *sent):
    count = hidden.shape[0]
    experts = len(sent)
    named = [routes[j : j + 1, :] for j in range(2)]
    memory = lax.broadcasted_iota(jnp.int32, (experts, count), 0)
    hits = [(memory == name).astype(jnp.float32) for name in named]
    rows = lax.broadcasted_iota(jnp.int32, (count, count), 0)
    cols = lax.broadcasted_iota(jnp.int32, (count, count), 1)
    earlier = jnp.where(rows < cols, 1.0, 0.0).astype(bf16)
    before = contract((hits[0] + hits[1]).astype(bf16), earlier, 1, 0)
    places = [jnp.sum(h * before, axis=0, keepdims=True).astype(jnp.int32) for h in hits]
    index = lax.broadcasted_iota(jnp.int32, (CAP, count), 0)
    crossed = [(name ^ here[1]) * CAP + place for name, place in zip(named, places)]
    for k in range(experts):
        at = index + k * CAP
        pick = jnp.where((at == crossed[0]) | (at == crossed[1]), 1.0, 0.0).astype(bf16)
        sent[k][...] = contract(pick, hidden[...], 1, 0).astype(bf16)
    slots = [(name * CAP + place).astype(jnp.float32) for name, place in zip(named, places)]
    level = levels[...].astype(jnp.float32)
    gates = level / (level[0:1, :] + level[1:2, :])
    entries = jnp.concatenate(slots + [gates, jnp.zeros((4, count), jnp.float32)], axis=0)
    table[...] = entries.T


def pack_kernel(here, *refs, plan, sources):
    weights, outs, sems = refs[:sources], refs[sources:-1], refs[-1]
    copies = []
    for i, ((source, start, step), out) in enumerate(zip(plan, outs)):
        at = pl.multiple_of(start + (here[1] & 3) * step, DK) if step else start
        cols = pl.ds(at, out.shape[1])
        ref = weights[source]
        view = ref.at[0, :, cols] if len(ref.shape) == 3 else ref.at[:, cols]
        copies.append(pltpu.make_async_copy(view, out, sems.at[i]))
    for copy in copies:
        copy.start()
    for copy in copies:
        copy.wait()


def join_kernel(here, *refs):
    *pieces, out = refs
    for k, piece in enumerate(pieces):
        out[pl.ds(pl.multiple_of((here[1] ^ k) * CAP, CAP), CAP), :] = piece[...]


def project(x, seq, pieces, masks):
    total = None
    for piece, mask in zip(pieces, masks):
        rows = piece.shape[0]
        at = pl.multiple_of((seq ^ mask) * rows, rows)
        part = contract(x[:, pl.ds(at, rows)], piece[...], 1, 0)
        total = part if total is None else total + part
    return total


def kv_kernel(here, x, *refs, masks):
    n = len(masks[0])
    k_out, v_out, t_out = refs[2 * n :]
    k_out[...] = project(x, here[0], refs[:n], masks[0]).astype(bf16)
    v_out[...] = project(x, here[0], refs[n : 2 * n], masks[1]).astype(bf16)
    for h in range(t_out.shape[0]):
        cols = slice(h * DK, (h + 1) * DK)
        t_out[h] = contract(k_out[:, cols], v_out[:, cols], 0, 0).astype(bf16)


def rows_kernel(here, *refs, masks):
    n = len(masks[0])
    out = refs[2 * n]
    at_col = 0
    for pieces, own in ((refs[:n], masks[0]), (refs[n : 2 * n], masks[1])):
        rows, cols = pieces[0].shape
        for piece, mask in zip(pieces, own):
            at = pl.multiple_of((here[0] ^ mask) * rows, rows)
            out[pl.ds(at, rows), at_col : at_col + cols] = piece[...]
        at_col += cols


def query_kernel(here, x, *refs):
    *quarters, out = refs
    for k, quarter in enumerate(quarters):
        cols = quarter.shape[1]
        at = pl.multiple_of(((here[1] & 3) ^ k) * cols, cols)
        out[:, pl.ds(at, cols)] = contract(x[...], quarter[...], 1, 0).astype(bf16)


def attend_kernel(here, q_all, k, v, *refs, first):
    *states, out = refs
    length = k.shape[0]
    step = length // 2
    row = lax.broadcasted_iota(jnp.int32, (step, step), 0)
    col = lax.broadcasted_iota(jnp.int32, (step, step), 1)
    causal = row >= col
    for head in range(states[0].shape[0]):
        cols = slice(head * DK, (head + 1) * DK)
        q_cols = slice((first + head) * DK, (first + head + 1) * DK)
        state = jnp.zeros((DK, DK), jnp.float32)
        for m, other in enumerate(states, 1):
            earlier = (here[0] ^ m) < here[0]
            state = state + jnp.where(earlier, other[head].astype(jnp.float32), 0.0)
        high = state.astype(bf16)
        low = (state - high.astype(jnp.float32)).astype(bf16)
        for b in range(2):
            rows = slice(b * step, (b + 1) * step)
            q = q_all[rows, q_cols]
            scores = jnp.where(causal, contract(q, k[rows, cols], 1, 1), 0.0).astype(bf16)
            reads = contract(scores, v[rows, cols], 1, 0)
            for e in range(b):
                before = slice(e * step, (e + 1) * step)
                scores = contract(q, k[before, cols], 1, 1).astype(bf16)
                reads = reads + contract(scores, v[before, cols], 1, 0)
            reads = reads + contract(q, high, 1, 0) + contract(q, low, 1, 0)
            scale = lax.rsqrt(jnp.mean(reads * reads, axis=-1, keepdims=True) + 1e-06)
            out[rows, cols] = (reads * scale).astype(bf16)


def combine_kernel(table, part, *refs):
    *prior, out = refs
    count = table.shape[0]
    at = 0
    for done in prior:
        out[:, : done.shape[1]] = done[...]
        at = done.shape[1]
    index = lax.broadcasted_iota(jnp.int32, (count, part.shape[0]), 1).astype(jnp.float32)
    mixed = None
    for j in range(2):
        pick = jnp.where(index == table[:, j : j + 1], 1.0, 0.0).astype(bf16)
        term = table[:, 2 + j : 3 + j] * contract(pick, part[...], 1, 0)
        mixed = term if mixed is None else mixed + term
    out[:, at:] = mixed.astype(bf16)


def call(kernel, outs, ins, *arrays, flops=1, scratch=(), last=False):
    arrays = [
        pltpu.with_memory_space_constraint(a, pltpu.VMEM) if spec is VMEM else a
        for a, spec in zip(arrays, ins)
    ]
    return pl.pallas_call(
        kernel,
        out_shape=outs if last else jax.tree.map(lambda s: pltpu.VMEM(s.shape, s.dtype), outs),
        in_specs=ins,
        out_specs=jax.tree.map(lambda _: VMEM, outs),
        scratch_shapes=scratch,
        compiler_params=pltpu.CompilerParams(vmem_limit_bytes=LIMIT),
        cost_estimate=pl.CostEstimate(flops=flops, bytes_accessed=1 << 20, transcendentals=0),
    )(*arrays)


def spread(first, bits):
    pieces, masks = [first], [0]
    for bit in bits:
        fresh = []
        for piece in pieces:
            fresh.append(swap(piece, "seq", bit))
        pieces = pieces + fresh
        masks = masks + [m ^ bit for m in masks]
    return pieces, tuple(masks)


def on_device(hidden, routes, gate_levels, query_weight, key_weight, value_weight):
    count, model = hidden.shape
    rows, width = query_weight.shape
    groups, experts = lax.axis_size("seq"), lax.axis_size("mem")
    here = jnp.stack([lax.axis_index("seq"), lax.axis_index("mem")]).astype(jnp.int32)
    bits = [1 << b for b in range(groups.bit_length() - 1)]
    length = experts * CAP
    all_heads = width // DK
    chunks = [(0, all_heads - LAST_HEADS), (all_heads - LAST_HEADS, LAST_HEADS)]

    def pack(plan):
        arrays = [query_weight, key_weight, value_weight]
        return call(
            functools.partial(pack_kernel, plan=[p[:3] for p in plan], sources=len(arrays)),
            [shape((rows, p[3]), bf16) for p in plan],
            [SMEM] + [HBM] * len(arrays),
            here,
            *[pltpu.with_memory_space_constraint(a, pltpu.HBM) for a in arrays],
            scratch=[pltpu.SemaphoreType.DMA((len(plan),))],
        )

    quarter = width // 4
    part = quarter // 2
    bound = chunks[0][1] * DK
    qa, qb = pack([(0, 0, quarter, part), (0, part, quarter, part)])
    k0, v0 = pack([(1, 0, 0, bound), (2, 0, 0, bound)])
    k1, v1 = pack([(1, bound, 0, width - bound), (2, bound, 0, width - bound)])
    qa_pieces, a_masks = spread(qa, bits)
    qb_pieces, b_masks = spread(qb, bits[::-1])
    masks = (a_masks, b_masks)
    weights = [(spread(k, bits)[0], spread(v, bits[::-1])[0]) for k, v in ((k0, v0), (k1, v1))]

    table, *sent = call(
        dispatch_kernel,
        [shape((count, 8), jnp.float32)] + [shape((CAP, model), bf16)] * experts,
        [SMEM, VMEM, VMEM, VMEM],
        here,
        routes.T,
        gate_levels.T,
        hidden,
        flops=2 * count * length * model,
    )

    def route(array, k):
        return swap(array, "mem", k)

    arrived = call(
        join_kernel,
        shape((length, model), bf16),
        [SMEM] + [VMEM] * experts,
        here,
        sent[0],
        *[route(sent[k], k) for k in range(1, experts)],
    )

    mine = call(
        functools.partial(rows_kernel, masks=masks),
        shape((model, quarter), bf16),
        [SMEM] + [VMEM] * (2 * groups),
        here,
        *qa_pieces,
        *qb_pieces,
    )
    quarter1 = swap(mine, "mem", 1)
    quarter2 = swap(mine, "mem", 2)
    quarter3 = swap(quarter2, "mem", 1)
    queries = call(
        query_kernel,
        shape((length, width), bf16),
        [SMEM] + [VMEM] * 5,
        here,
        arrived,
        mine,
        quarter1,
        quarter2,
        quarter3,
        flops=2 * length * model * width,
    )

    out = None
    for c, (first, heads) in enumerate(chunks):
        cols = heads * DK
        keys, values, total = call(
            functools.partial(kv_kernel, masks=masks),
            [
                shape((length, cols), bf16),
                shape((length, cols), bf16),
                shape((heads, DK, DK), bf16),
            ],
            [SMEM, VMEM] + [VMEM] * (2 * groups),
            here,
            arrived,
            *weights[c][0],
            *weights[c][1],
            flops=4 * length * model * cols,
        )
        states = []
        for m in range(1, groups):
            states.append(swap(total, "seq", m))
        normed = call(
            functools.partial(attend_kernel, first=first),
            shape((length, cols), bf16),
            [SMEM] + [VMEM] * (3 + len(states)),
            here,
            queries,
            keys,
            values,
            *states,
            flops=4 * length * length * cols,
        )
        back = lax.all_to_all(
            normed.reshape(experts, CAP, cols), "mem", split_axis=0, concat_axis=0, tiled=True
        )
        back = back.reshape(length, cols)
        prior = [] if out is None else [out]
        out = call(
            combine_kernel,
            shape((count, first * DK + cols), bf16),
            [VMEM] * (2 + len(prior)),
            table,
            back,
            *prior,
            last=c + 1 == len(chunks),
        )
    return out


def solution(mesh):
    return jax.shard_map(
        on_device,
        mesh=mesh,
        in_specs=(
            P(("seq", "mem"), None),
            P(("seq", "mem"), None),
            P(("seq", "mem"), None),
            P("seq", None),
            P("mem", "seq", None),
            P("mem", "seq", None),
        ),
        out_specs=P(("seq", "mem"), None),
        check_vma=False,
    )
```

```python
import functools

import jax
import jax.numpy as jnp
from jax import lax
from jax.experimental import pallas as pl
from jax.experimental.pallas import tpu as pltpu
from jax.sharding import PartitionSpec as P


DK = 128
CAP = 64
LAST_HEADS = 2
PIECES = (True, True)
EARLY = (True, False)
LIMIT = 24 << 20
VMEM = pl.BlockSpec(memory_space=pltpu.VMEM)
SMEM = pl.BlockSpec(memory_space=pltpu.SMEM)
ANY = pl.BlockSpec(memory_space=pl.ANY)
HBM = pl.BlockSpec(memory_space=pltpu.HBM)
shape = jax.ShapeDtypeStruct
bf16 = jnp.bfloat16


def swap(array, axis, mask):
    return lax.ppermute(array, axis, [(i, i ^ mask) for i in range(lax.axis_size(axis))])


def contract(left, right, left_dim, right_dim):
    return lax.dot_general(
        left, right, (((left_dim,), (right_dim,)), ((), ())), preferred_element_type=jnp.float32
    )


def dispatch_kernel(here, routes, levels, hidden, table, *sent):
    count = hidden.shape[0]
    experts = len(sent)
    named = [routes[j : j + 1, :] for j in range(2)]
    memory = lax.broadcasted_iota(jnp.int32, (experts, count), 0)
    hits = [(memory == name).astype(jnp.float32) for name in named]
    rows = lax.broadcasted_iota(jnp.int32, (count, count), 0)
    cols = lax.broadcasted_iota(jnp.int32, (count, count), 1)
    earlier = jnp.where(rows < cols, 1.0, 0.0).astype(bf16)
    before = contract((hits[0] + hits[1]).astype(bf16), earlier, 1, 0)
    places = [jnp.sum(h * before, axis=0, keepdims=True).astype(jnp.int32) for h in hits]
    index = lax.broadcasted_iota(jnp.int32, (CAP, count), 0)
    crossed = [(name ^ here[1]) * CAP + place for name, place in zip(named, places)]
    for k in range(experts):
        at = index + k * CAP
        pick = jnp.where((at == crossed[0]) | (at == crossed[1]), 1.0, 0.0).astype(bf16)
        sent[k][...] = contract(pick, hidden[...], 1, 0).astype(bf16)
    slots = [(name * CAP + place).astype(jnp.float32) for name, place in zip(named, places)]
    level = levels[...].astype(jnp.float32)
    gates = level / (level[0:1, :] + level[1:2, :])
    turned = [c.astype(jnp.float32) for c in crossed]
    entries = jnp.concatenate(slots + [gates] + turned + [jnp.zeros((2, count), jnp.float32)], axis=0)
    table[...] = entries.T


def pack_kernel(here, *refs, plan, sources):
    weights, outs, sems = refs[:sources], refs[sources:-1], refs[-1]
    copies = []
    for i, ((source, start, step), out) in enumerate(zip(plan, outs)):
        at = pl.multiple_of(start + (here[1] & 3) * step, DK) if step else start
        cols = pl.ds(at, out.shape[1])
        ref = weights[source]
        view = ref.at[0, :, cols] if len(ref.shape) == 3 else ref.at[:, cols]
        copies.append(pltpu.make_async_copy(view, out, sems.at[i]))
    for copy in copies:
        copy.start()
    for copy in copies:
        copy.wait()


def join_kernel(here, *refs):
    *pieces, out = refs
    for k, piece in enumerate(pieces):
        out[pl.ds(pl.multiple_of((here[1] ^ k) * CAP, CAP), CAP), :] = piece[...]


def project(x, seq, pieces, masks):
    total = None
    for piece, mask in zip(pieces, masks):
        rows = piece.shape[0]
        at = pl.multiple_of((seq ^ mask) * rows, rows)
        part = contract(x[:, pl.ds(at, rows)], piece[...], 1, 0)
        total = part if total is None else total + part
    return total


def early_kernel(here, x, *refs, masks):
    n = len(masks[0])
    k_out, v_out = refs[2 * n :]
    k_out[...] = project(x, here[0], refs[:n], masks[0])
    v_out[...] = project(x, here[0], refs[n : 2 * n], masks[1])


def kv_kernel(here, x, *refs, masks, early):
    n = len(masks[0])
    partial = refs[2 * n : 2 * n + early]
    k_out, v_out, t_out = refs[2 * n + early :]
    for s, out in enumerate((k_out, v_out)):
        total = project(x, here[0], refs[s * n : (s + 1) * n], masks[s])
        if early:
            total = total + partial[s][...]
        out[...] = total.astype(bf16)
    for h in range(t_out.shape[0]):
        cols = slice(h * DK, (h + 1) * DK)
        t_out[h] = contract(k_out[:, cols], v_out[:, cols], 0, 0).astype(bf16)


def rows_kernel(here, *refs, masks):
    n = len(masks[0])
    out = refs[2 * n]
    at_col = 0
    for pieces, own in ((refs[:n], masks[0]), (refs[n : 2 * n], masks[1])):
        rows, cols = pieces[0].shape
        for piece, mask in zip(pieces, own):
            at = pl.multiple_of((here[0] ^ mask) * rows, rows)
            out[pl.ds(at, rows), at_col : at_col + cols] = piece[...]
        at_col += cols


def query_kernel(here, x, *refs):
    *quarters, out = refs
    for k, quarter in enumerate(quarters):
        cols = quarter.shape[1]
        at = pl.multiple_of(((here[1] & 3) ^ k) * cols, cols)
        out[:, pl.ds(at, cols)] = contract(x[...], quarter[...], 1, 0).astype(bf16)


def attend_kernel(here, q_all, k, v, *refs, first, others):
    states, outs = refs[:others], refs[others:]
    length = k.shape[0]
    if len(outs) > 1:
        *outs, out = outs
    else:
        (out,), outs = outs, []
    step = length // 2
    row = lax.broadcasted_iota(jnp.int32, (step, step), 0)
    col = lax.broadcasted_iota(jnp.int32, (step, step), 1)
    causal = row >= col
    for head in range(states[0].shape[0]):
        cols = slice(head * DK, (head + 1) * DK)
        q_cols = slice((first + head) * DK, (first + head + 1) * DK)
        state = jnp.zeros((DK, DK), jnp.float32)
        for m, other in enumerate(states, 1):
            earlier = (here[0] ^ m) < here[0]
            state = state + jnp.where(earlier, other[head].astype(jnp.float32), 0.0)
        high = state.astype(bf16)
        low = (state - high.astype(jnp.float32)).astype(bf16)
        for b in range(2):
            rows = slice(b * step, (b + 1) * step)
            q = q_all[rows, q_cols]
            scores = jnp.where(causal, contract(q, k[rows, cols], 1, 1), 0.0).astype(bf16)
            reads = contract(scores, v[rows, cols], 1, 0)
            for e in range(b):
                before = slice(e * step, (e + 1) * step)
                scores = contract(q, k[before, cols], 1, 1).astype(bf16)
                reads = reads + contract(scores, v[before, cols], 1, 0)
            reads = reads + contract(q, high, 1, 0) + contract(q, low, 1, 0)
            scale = lax.rsqrt(jnp.mean(reads * reads, axis=-1, keepdims=True) + 1e-06)
            out[rows, cols] = (reads * scale).astype(bf16)
    for k, piece in enumerate(outs):
        piece[...] = out[pl.ds(pl.multiple_of((here[1] ^ k) * CAP, CAP), CAP), :]


def combine_kernel(table, *refs, parts, at):
    pieces, prior, out = refs[:parts], refs[parts:-1], refs[-1]
    count = table.shape[0]
    for done in prior:
        out[:, :at] = done[...]
    part = jnp.concatenate([p[...] for p in pieces], axis=0)
    index = lax.broadcasted_iota(jnp.int32, (count, part.shape[0]), 1).astype(jnp.float32)
    column = 4 if parts > 1 else 0
    mixed = None
    for j in range(2):
        pick = jnp.where(index == table[:, column + j : column + j + 1], 1.0, 0.0).astype(bf16)
        term = table[:, 2 + j : 3 + j] * contract(pick, part, 1, 0)
        mixed = term if mixed is None else mixed + term
    out[:, at:] = mixed.astype(bf16)


def call(kernel, outs, ins, *arrays, flops=1, scratch=(), last=False):
    arrays = [
        pltpu.with_memory_space_constraint(a, pltpu.VMEM) if spec is VMEM else a
        for a, spec in zip(arrays, ins)
    ]
    return pl.pallas_call(
        kernel,
        out_shape=outs if last else jax.tree.map(lambda s: pltpu.VMEM(s.shape, s.dtype), outs),
        in_specs=ins,
        out_specs=jax.tree.map(lambda _: VMEM, outs),
        scratch_shapes=scratch,
        compiler_params=pltpu.CompilerParams(vmem_limit_bytes=LIMIT),
        cost_estimate=pl.CostEstimate(flops=flops, bytes_accessed=1 << 20, transcendentals=0),
    )(*arrays)


def spread(first, bits):
    pieces, masks = [first], [0]
    for bit in bits:
        fresh = []
        for piece in pieces:
            fresh.append(swap(piece, "seq", bit))
        pieces = pieces + fresh
        masks = masks + [m ^ bit for m in masks]
    return pieces, tuple(masks)


def on_device(hidden, routes, gate_levels, query_weight, key_weight, value_weight):
    count, model = hidden.shape
    rows, width = query_weight.shape
    groups, experts = lax.axis_size("seq"), lax.axis_size("mem")
    here = jnp.stack([lax.axis_index("seq"), lax.axis_index("mem")]).astype(jnp.int32)
    bits = [1 << b for b in range(groups.bit_length() - 1)]
    length = experts * CAP
    all_heads = width // DK
    chunks = [(0, all_heads - LAST_HEADS), (all_heads - LAST_HEADS, LAST_HEADS)]

    def pack(plan):
        arrays = [query_weight, key_weight, value_weight]
        return call(
            functools.partial(pack_kernel, plan=[p[:3] for p in plan], sources=len(arrays)),
            [shape((rows, p[3]), bf16) for p in plan],
            [SMEM] + [HBM] * len(arrays),
            here,
            *[pltpu.with_memory_space_constraint(a, pltpu.HBM) for a in arrays],
            scratch=[pltpu.SemaphoreType.DMA((len(plan),))],
        )

    quarter = width // 4
    part = quarter // 2
    bound = chunks[0][1] * DK
    qa, qb = pack([(0, 0, quarter, part), (0, part, quarter, part)])
    k0, v0 = pack([(1, 0, 0, bound), (2, 0, 0, bound)])
    k1, v1 = pack([(1, bound, 0, width - bound), (2, bound, 0, width - bound)])
    qa_pieces, a_masks = spread(qa, bits)
    qb_pieces, b_masks = spread(qb, bits[::-1])
    masks = (a_masks, b_masks)
    weights = [(spread(k, bits)[0], spread(v, bits[::-1])[0]) for k, v in ((k0, v0), (k1, v1))]

    table, *sent = call(
        dispatch_kernel,
        [shape((count, 8), jnp.float32)] + [shape((CAP, model), bf16)] * experts,
        [SMEM, VMEM, VMEM, VMEM],
        here,
        routes.T,
        gate_levels.T,
        hidden,
        flops=2 * count * length * model,
    )

    def route(array, k):
        return swap(array, "mem", k)

    arrived = call(
        join_kernel,
        shape((length, model), bf16),
        [SMEM] + [VMEM] * experts,
        here,
        sent[0],
        *[route(sent[k], k) for k in range(1, experts)],
    )

    mine = call(
        functools.partial(rows_kernel, masks=masks),
        shape((model, quarter), bf16),
        [SMEM] + [VMEM] * (2 * groups),
        here,
        *qa_pieces,
        *qb_pieces,
    )
    quarter1 = swap(mine, "mem", 1)
    quarter2 = swap(mine, "mem", 2)
    quarter3 = swap(quarter2, "mem", 1)
    queries = call(
        query_kernel,
        shape((length, width), bf16),
        [SMEM] + [VMEM] * 5,
        here,
        arrived,
        mine,
        quarter1,
        quarter2,
        quarter3,
        flops=2 * length * model * width,
    )

    out = None
    for c, (first, heads) in enumerate(chunks):
        cols = heads * DK
        k_pieces, v_pieces = weights[c]
        near = groups // 2 + 1 if EARLY[c] else 0
        partial = []
        if near:
            partial = call(
                functools.partial(early_kernel, masks=[m[:near] for m in masks]),
                [shape((length, cols), jnp.float32)] * 2,
                [SMEM] + [VMEM] * (1 + 2 * near),
                here,
                arrived,
                *k_pieces[:near],
                *v_pieces[:near],
                flops=3 * length * model * cols,
            )
        keys, values, total = call(
            functools.partial(kv_kernel, masks=[m[near:] for m in masks], early=len(partial)),
            [
                shape((length, cols), bf16),
                shape((length, cols), bf16),
                shape((heads, DK, DK), bf16),
            ],
            [SMEM] + [VMEM] * (1 + 2 * (groups - near) + len(partial)),
            here,
            arrived,
            *k_pieces[near:],
            *v_pieces[near:],
            *partial,
            flops=4 * length * model * cols,
        )
        states = []
        for m in range(1, groups):
            states.append(swap(total, "seq", m))
        pieces = experts if PIECES[c] else 1
        normed = call(
            functools.partial(attend_kernel, first=first, others=len(states)),
            [shape((length // pieces, cols), bf16)] * pieces,
            [SMEM] + [VMEM] * (3 + len(states)),
            here,
            queries,
            keys,
            values,
            *states,
            flops=4 * length * length * cols,
            scratch=[pltpu.VMEM((length, cols), bf16)] if pieces > 1 else [],
        )
        if pieces > 1:
            back = [normed[0]]
            for k in range(1, experts):
                back.append(swap(normed[k], "mem", k))
        else:
            back = [
                lax.all_to_all(
                    normed[0].reshape(experts, CAP, cols), "mem", split_axis=0, concat_axis=0, tiled=True
                ).reshape(length, cols)
            ]
        prior = [] if out is None else [out]
        out = call(
            functools.partial(combine_kernel, parts=len(back), at=first * DK),
            shape((count, first * DK + cols), bf16),
            [VMEM] * (1 + len(back) + len(prior)),
            table,
            *back,
            *prior,
            last=c + 1 == len(chunks),
        )
    return out


def solution(mesh):
    return jax.shard_map(
        on_device,
        mesh=mesh,
        in_specs=(
            P(("seq", "mem"), None),
            P(("seq", "mem"), None),
            P(("seq", "mem"), None),
            P("seq", None),
            P("mem", "seq", None),
            P("mem", "seq", None),
        ),
        out_specs=P(("seq", "mem"), None),
        check_vma=False,
    )
```

```python
import functools

import jax
import jax.numpy as jnp
from jax import lax
from jax.experimental import pallas as pl
from jax.experimental.pallas import tpu as pltpu
from jax.sharding import PartitionSpec as P


DK = 128
CAP = 64
LAST_HEADS = 2
EARLY = (True, False)
LIMIT = 24 << 20
VMEM = pl.BlockSpec(memory_space=pltpu.VMEM)
SMEM = pl.BlockSpec(memory_space=pltpu.SMEM)
ANY = pl.BlockSpec(memory_space=pl.ANY)
HBM = pl.BlockSpec(memory_space=pltpu.HBM)
shape = jax.ShapeDtypeStruct
bf16 = jnp.bfloat16


def swap(array, axis, mask):
    return lax.ppermute(array, axis, [(i, i ^ mask) for i in range(lax.axis_size(axis))])


def contract(left, right, left_dim, right_dim):
    return lax.dot_general(
        left, right, (((left_dim,), (right_dim,)), ((), ())), preferred_element_type=jnp.float32
    )


def dispatch_kernel(here, routes, levels, hidden, table, *sent):
    count = hidden.shape[0]
    experts = len(sent)
    named = [routes[j : j + 1, :] for j in range(2)]
    memory = lax.broadcasted_iota(jnp.int32, (experts, count), 0)
    hits = [(memory == name).astype(jnp.float32) for name in named]
    rows = lax.broadcasted_iota(jnp.int32, (count, count), 0)
    cols = lax.broadcasted_iota(jnp.int32, (count, count), 1)
    earlier = jnp.where(rows < cols, 1.0, 0.0).astype(bf16)
    before = contract((hits[0] + hits[1]).astype(bf16), earlier, 1, 0)
    places = [jnp.sum(h * before, axis=0, keepdims=True).astype(jnp.int32) for h in hits]
    index = lax.broadcasted_iota(jnp.int32, (CAP, count), 0)
    crossed = [(name ^ here[1]) * CAP + place for name, place in zip(named, places)]
    for k in range(experts):
        at = index + k * CAP
        pick = jnp.where((at == crossed[0]) | (at == crossed[1]), 1.0, 0.0).astype(bf16)
        sent[k][...] = contract(pick, hidden[...], 1, 0).astype(bf16)
    slots = [c.astype(jnp.float32) for c in crossed]
    level = levels[...].astype(jnp.float32)
    gates = level / (level[0:1, :] + level[1:2, :])
    entries = jnp.concatenate(slots + [gates, jnp.zeros((4, count), jnp.float32)], axis=0)
    table[...] = entries.T


def pack_kernel(here, *refs, plan, sources):
    weights, outs, sems = refs[:sources], refs[sources:-1], refs[-1]
    copies = []
    for i, ((source, start, step), out) in enumerate(zip(plan, outs)):
        at = pl.multiple_of(start + (here[1] & 3) * step, DK) if step else start
        cols = pl.ds(at, out.shape[1])
        ref = weights[source]
        view = ref.at[0, :, cols] if len(ref.shape) == 3 else ref.at[:, cols]
        copies.append(pltpu.make_async_copy(view, out, sems.at[i]))
    for copy in copies:
        copy.start()
    for copy in copies:
        copy.wait()


def join_kernel(here, *refs):
    *pieces, out = refs
    for k, piece in enumerate(pieces):
        out[pl.ds(pl.multiple_of((here[1] ^ k) * CAP, CAP), CAP), :] = piece[...]


def project(x, seq, pieces, masks):
    total = None
    for piece, mask in zip(pieces, masks):
        rows = piece.shape[0]
        at = pl.multiple_of((seq ^ mask) * rows, rows)
        part = contract(x[:, pl.ds(at, rows)], piece[...], 1, 0)
        total = part if total is None else total + part
    return total


def early_kernel(here, x, *refs, masks):
    n = len(masks[0])
    k_out, v_out = refs[2 * n :]
    k_out[...] = project(x, here[0], refs[:n], masks[0])
    v_out[...] = project(x, here[0], refs[n : 2 * n], masks[1])


def kv_kernel(here, x, *refs, masks, early):
    n = len(masks[0])
    partial = refs[2 * n : 2 * n + early]
    k_out, v_out, t_out = refs[2 * n + early :]
    for s, out in enumerate((k_out, v_out)):
        total = project(x, here[0], refs[s * n : (s + 1) * n], masks[s])
        if early:
            total = total + partial[s][...]
        out[...] = total.astype(bf16)
    for h in range(t_out.shape[0]):
        cols = slice(h * DK, (h + 1) * DK)
        t_out[h] = contract(k_out[:, cols], v_out[:, cols], 0, 0).astype(bf16)


def rows_kernel(here, *refs, masks):
    n = len(masks[0])
    out = refs[2 * n]
    at_col = 0
    for pieces, own in ((refs[:n], masks[0]), (refs[n : 2 * n], masks[1])):
        rows, cols = pieces[0].shape
        for piece, mask in zip(pieces, own):
            at = pl.multiple_of((here[0] ^ mask) * rows, rows)
            out[pl.ds(at, rows), at_col : at_col + cols] = piece[...]
        at_col += cols


def near_query_kernel(x, *refs):
    *quarters, out = refs
    for k, quarter in enumerate(quarters):
        cols = quarter.shape[1]
        out[:, k * cols : (k + 1) * cols] = contract(x[...], quarter[...], 1, 0).astype(bf16)


def query_kernel(here, x, near, *refs):
    *quarters, out = refs
    cols = quarters[0].shape[1]
    known = near.shape[1] // cols
    for k in range(known + len(quarters)):
        at = pl.multiple_of(((here[1] & 3) ^ k) * cols, cols)
        if k < known:
            out[:, pl.ds(at, cols)] = near[:, k * cols : (k + 1) * cols]
        else:
            out[:, pl.ds(at, cols)] = contract(x[...], quarters[k - known][...], 1, 0).astype(bf16)


def local_kernel(q_all, k, v, reads, *, first):
    step = k.shape[0] // 2
    row = lax.broadcasted_iota(jnp.int32, (step, step), 0)
    col = lax.broadcasted_iota(jnp.int32, (step, step), 1)
    causal = row >= col
    for head in range(k.shape[1] // DK):
        cols = slice(head * DK, (head + 1) * DK)
        q_cols = slice((first + head) * DK, (first + head + 1) * DK)
        for b in range(2):
            rows = slice(b * step, (b + 1) * step)
            q = q_all[rows, q_cols]
            scores = jnp.where(causal, contract(q, k[rows, cols], 1, 1), 0.0).astype(bf16)
            total = contract(scores, v[rows, cols], 1, 0)
            for e in range(b):
                before = slice(e * step, (e + 1) * step)
                scores = contract(q, k[before, cols], 1, 1).astype(bf16)
                total = total + contract(scores, v[before, cols], 1, 0)
            reads[rows, cols] = total


def attend_kernel(here, q_all, reads, *refs, first, others):
    states, outs, out = refs[:others], refs[others:-1], refs[-1]
    for head in range(states[0].shape[0]):
        cols = slice(head * DK, (head + 1) * DK)
        q = q_all[:, (first + head) * DK : (first + head + 1) * DK]
        state = jnp.zeros((DK, DK), jnp.float32)
        for m, other in enumerate(states, 1):
            earlier = (here[0] ^ m) < here[0]
            state = state + jnp.where(earlier, other[head].astype(jnp.float32), 0.0)
        high = state.astype(bf16)
        low = (state - high.astype(jnp.float32)).astype(bf16)
        total = reads[:, cols] + contract(q, high, 1, 0) + contract(q, low, 1, 0)
        scale = lax.rsqrt(jnp.mean(total * total, axis=-1, keepdims=True) + 1e-06)
        out[:, cols] = (total * scale).astype(bf16)
    for k, piece in enumerate(outs):
        piece[...] = out[pl.ds(pl.multiple_of((here[1] ^ k) * CAP, CAP), CAP), :]


def combine_kernel(table, *refs, parts, at):
    pieces, prior, out = refs[:parts], refs[parts:-1], refs[-1]
    count = table.shape[0]
    for done in prior:
        out[:, :at] = done[...]
    part = jnp.concatenate([p[...] for p in pieces], axis=0)
    index = lax.broadcasted_iota(jnp.int32, (count, part.shape[0]), 1).astype(jnp.float32)
    mixed = None
    for j in range(2):
        pick = jnp.where(index == table[:, j : j + 1], 1.0, 0.0).astype(bf16)
        term = table[:, 2 + j : 3 + j] * contract(pick, part, 1, 0)
        mixed = term if mixed is None else mixed + term
    out[:, at:] = mixed.astype(bf16)


def call(kernel, outs, ins, *arrays, flops=1, scratch=(), last=False):
    arrays = [
        pltpu.with_memory_space_constraint(a, pltpu.VMEM) if spec is VMEM else a
        for a, spec in zip(arrays, ins)
    ]
    return pl.pallas_call(
        kernel,
        out_shape=outs if last else jax.tree.map(lambda s: pltpu.VMEM(s.shape, s.dtype), outs),
        in_specs=ins,
        out_specs=jax.tree.map(lambda _: VMEM, outs),
        scratch_shapes=scratch,
        compiler_params=pltpu.CompilerParams(vmem_limit_bytes=LIMIT),
        cost_estimate=pl.CostEstimate(flops=flops, bytes_accessed=1 << 20, transcendentals=0),
    )(*arrays)


def spread(first, bits):
    pieces, masks = [first], [0]
    for bit in bits:
        fresh = []
        for piece in pieces:
            fresh.append(swap(piece, "seq", bit))
        pieces = pieces + fresh
        masks = masks + [m ^ bit for m in masks]
    return pieces, tuple(masks)


def on_device(hidden, routes, gate_levels, query_weight, key_weight, value_weight):
    count, model = hidden.shape
    rows, width = query_weight.shape
    groups, experts = lax.axis_size("seq"), lax.axis_size("mem")
    here = jnp.stack([lax.axis_index("seq"), lax.axis_index("mem")]).astype(jnp.int32)
    bits = [1 << b for b in range(groups.bit_length() - 1)]
    length = experts * CAP
    all_heads = width // DK
    chunks = [(0, all_heads - LAST_HEADS), (all_heads - LAST_HEADS, LAST_HEADS)]

    def pack(plan):
        arrays = [query_weight, key_weight, value_weight]
        return call(
            functools.partial(pack_kernel, plan=[p[:3] for p in plan], sources=len(arrays)),
            [shape((rows, p[3]), bf16) for p in plan],
            [SMEM] + [HBM] * len(arrays),
            here,
            *[pltpu.with_memory_space_constraint(a, pltpu.HBM) for a in arrays],
            scratch=[pltpu.SemaphoreType.DMA((len(plan),))],
        )

    quarter = width // 4
    part = quarter // 2
    bound = chunks[0][1] * DK
    qa, qb = pack([(0, 0, quarter, part), (0, part, quarter, part)])
    k0, v0 = pack([(1, 0, 0, bound), (2, 0, 0, bound)])
    k1, v1 = pack([(1, bound, 0, width - bound), (2, bound, 0, width - bound)])
    qa_pieces, a_masks = spread(qa, bits)
    qb_pieces, b_masks = spread(qb, bits[::-1])
    masks = (a_masks, b_masks)
    weights = [(spread(k, bits)[0], spread(v, bits[::-1])[0]) for k, v in ((k0, v0), (k1, v1))]

    table, *sent = call(
        dispatch_kernel,
        [shape((count, 8), jnp.float32)] + [shape((CAP, model), bf16)] * experts,
        [SMEM, VMEM, VMEM, VMEM],
        here,
        routes.T,
        gate_levels.T,
        hidden,
        flops=2 * count * length * model,
    )

    def route(array, k):
        return swap(array, "mem", k)

    arrived = call(
        join_kernel,
        shape((length, model), bf16),
        [SMEM] + [VMEM] * experts,
        here,
        sent[0],
        *[route(sent[k], k) for k in range(1, experts)],
    )

    mine = call(
        functools.partial(rows_kernel, masks=masks),
        shape((model, quarter), bf16),
        [SMEM] + [VMEM] * (2 * groups),
        here,
        *qa_pieces,
        *qb_pieces,
    )
    quarter1 = swap(mine, "mem", 1)
    quarter2 = swap(mine, "mem", 2)
    quarter3 = swap(quarter2, "mem", 1)
    near_queries = call(
        near_query_kernel,
        shape((length, 2 * quarter), bf16),
        [VMEM] * 3,
        arrived,
        mine,
        quarter1,
        flops=length * model * width,
    )
    queries = call(
        query_kernel,
        shape((length, width), bf16),
        [SMEM] + [VMEM] * 4,
        here,
        arrived,
        near_queries,
        quarter2,
        quarter3,
        flops=length * model * width,
    )

    out = None
    for c, (first, heads) in enumerate(chunks):
        cols = heads * DK
        k_pieces, v_pieces = weights[c]
        near = groups // 2 + 1 if EARLY[c] else 0
        partial = []
        if near:
            partial = call(
                functools.partial(early_kernel, masks=[m[:near] for m in masks]),
                [shape((length, cols), jnp.float32)] * 2,
                [SMEM] + [VMEM] * (1 + 2 * near),
                here,
                arrived,
                *k_pieces[:near],
                *v_pieces[:near],
                flops=3 * length * model * cols,
            )
        keys, values, total = call(
            functools.partial(kv_kernel, masks=[m[near:] for m in masks], early=len(partial)),
            [
                shape((length, cols), bf16),
                shape((length, cols), bf16),
                shape((heads, DK, DK), bf16),
            ],
            [SMEM] + [VMEM] * (1 + 2 * (groups - near) + len(partial)),
            here,
            arrived,
            *k_pieces[near:],
            *v_pieces[near:],
            *partial,
            flops=4 * length * model * cols,
        )
        states = []
        for m in range(1, groups):
            states.append(swap(total, "seq", m))
        reads = call(
            functools.partial(local_kernel, first=first),
            shape((length, cols), jnp.float32),
            [VMEM] * 3,
            queries,
            keys,
            values,
            flops=3 * length * length * cols,
        )
        normed = call(
            functools.partial(attend_kernel, first=first, others=len(states)),
            [shape((CAP, cols), bf16)] * experts,
            [SMEM] + [VMEM] * (2 + len(states)),
            here,
            queries,
            reads,
            *states,
            flops=4 * length * DK * cols,
            scratch=[pltpu.VMEM((length, cols), bf16)],
        )
        back = [normed[0]]
        for k in range(1, experts):
            back.append(swap(normed[k], "mem", k))
        prior = [] if out is None else [out]
        out = call(
            functools.partial(combine_kernel, parts=len(back), at=first * DK),
            shape((count, first * DK + cols), bf16),
            [VMEM] * (1 + len(back) + len(prior)),
            table,
            *back,
            *prior,
            last=c + 1 == len(chunks),
        )
    return out


def solution(mesh):
    return jax.shard_map(
        on_device,
        mesh=mesh,
        in_specs=(
            P(("seq", "mem"), None),
            P(("seq", "mem"), None),
            P(("seq", "mem"), None),
            P("seq", None),
            P("mem", "seq", None),
            P("mem", "seq", None),
        ),
        out_specs=P(("seq", "mem"), None),
        check_vma=False,
    )
```
